512 devices in a mesh: groups: 2 (over y), range: 128 (over z, x), sub: 2 (over core).
Axes of the slice: x: 8, y: 2, z: 16, core: 2. Of those that a mesh axis runs over, the one named last changes fastest.
The devices are a block of a 8x8x16 slice.
Arguments:
- samples: float32 [2, 1024, 512, 128], P(None, ('groups', 'range', 'sub')), parts along dimension 1, may hold values from -6 to 6
- beam_weights: float32 [512, 8, 2, 64, 128], P(('groups', 'range'), None, None, None, 'sub'), parts along dimension 0, may hold values from -0.25 to 0.25
- subarrays: int32 [512, 8, 64], P(('groups', 'range', 'sub')), parts along dimension 0, may hold values from 0 to 511, as said below
- training: int32 [1024], P(('groups', 'range', 'sub')), parts along dimension 0, may hold values 0 or 1
Outputs:
- covariance: float32 [512, 8, 64, 128], P(('groups', 'range', 'sub')), parts along dimension 0
- filtered: float32 [2, 128, 1024, 128], P(None, None, ('groups', 'range', 'sub')), parts along dimension 2
- energy: float32 [256], P('groups'), parts along dimension 0
The draws below stay inside these ranges and needn't reach their ends.
There are 2 independent parts, one for each index of `groups`. The reference program is written for one: setup_inputs(seed, part) draws one part's arguments, and reference() takes and returns one part's arrays. A program takes and returns all parts, laid end to end along the dimension named above; each array names one. Nothing has to cross between parts.
Inputs may be any that keep to these rules, and one draw needn't show every extreme that they name: `subarrays`: in each gate block the 512 indices are all 512 channels, each once.
All inputs are finite; a program needn't handle non-finite values. No bound on the sum of `training` on one device may be relied on, other than what follows from the above.
Results may differ from the reference program's by a relative error of at most 0.0003.
Values sent between devices are 32-bit elements; how exact they have to be, the bound alone decides.
A program may use at most 64 MiB of HBM per device.

```python
import jax
import jax.numpy as jnp
from jax import lax

C = 512
S = 64
K = 128
P_SIZE = 128
GB = 2
NS = 8
G = 512
NB = 256


def draw_subarrays(key, part):
    several = jax.random.split(jax.random.fold_in(key, 17), NB)
    orders = jax.vmap(lambda single: jax.random.permutation(single, C))(several)
    return orders.reshape(NB, NS, S).astype(jnp.int32)


def plant(values, stream_key, smallest, top_value):
    longest = values.shape.index(max(values.shape))
    spots = []
    for shift in (0, 1):
        where = [jax.random.randint(jax.random.fold_in(stream_key, axis), (), 0, length) for axis, length in enumerate(values.shape)]
        where[longest] = (where[longest] + shift) % values.shape[longest]
        spots.append(tuple(where))
    return values.at[spots[0]].set(smallest).at[spots[1]].set(top_value)


def level_of(rng, extent, cuts, least, high):
    level, own = 1.0, jax.random.fold_in(rng, 6)
    for dim, parts in cuts:
        heights = jnp.exp(jax.random.uniform(jax.random.fold_in(own, dim), (parts,), jnp.float32, least / len(cuts), high / len(cuts)))
        level = level * jnp.repeat(heights, extent[dim] // parts).reshape([-1 if axis == dim else 1 for axis in range(len(extent))])
    return level


def normal_values(key, extent, width, bound, cuts=(), kind=jnp.bfloat16):
    drawn = width * jax.random.normal(key, extent, jnp.float32)
    if cuts:
        drawn = drawn * level_of(key, extent, cuts, -0.22, 0.18)
    return jnp.clip(drawn, -bound, bound).astype(kind)


def setup_inputs(seed: int = 0, part: int = 0) -> dict:
    splits = jax.random.split(jax.random.key(seed), 5)
    part_keys = jax.random.split(jax.random.fold_in(splits[4], part), 5)
    samples = normal_values(part_keys[0], (2, C, G, P_SIZE), 1.0, 6.0, ((1, 256),), jnp.float32)
    beam_weights = normal_values(part_keys[1], (NB, NS, 2, S, K), C ** -0.5, 0.25, ((0, 128), (4, 2)), jnp.float32)
    subarrays = draw_subarrays(jax.random.fold_in(jax.random.fold_in(splits[4], part), 71), part)
    training = plant((jax.random.randint(part_keys[3], (G,), 0, 2) < 1).astype(jnp.int32), jax.random.fold_in(part_keys[3], 1), 0, 1)
    return dict(samples=samples, beam_weights=beam_weights, subarrays=subarrays, training=training)


loading = 0.05

def block_terms(snaps, chosen, weights, masked, factor):
    highest = lax.Precision.HIGHEST
    picked = jnp.take(snaps, chosen, axis=1)
    real_part = picked[0]
    imag_part = picked[1]
    real_masked = real_part * masked
    imag_masked = imag_part * masked
    cov_real = (jnp.einsum('snx,smx->snm', real_masked, real_part, precision=highest) + jnp.einsum('snx,smx->snm', imag_masked, imag_part, precision=highest)) * factor
    cov_imag = (jnp.einsum('snx,smx->snm', imag_masked, real_part, precision=highest) - jnp.einsum('snx,smx->snm', real_masked, imag_part, precision=highest)) * factor
    w_real = weights[:, 0]
    w_imag = weights[:, 1]
    out_real = jnp.einsum('snk,snx->kx', w_real, real_part, precision=highest) + jnp.einsum('snk,snx->kx', w_imag, imag_part, precision=highest)
    out_imag = jnp.einsum('snk,snx->kx', w_real, imag_part, precision=highest) - jnp.einsum('snk,snx->kx', w_imag, real_part, precision=highest)
    prod_real = jnp.einsum('snm,smk->snk', cov_real, w_real, precision=highest) - jnp.einsum('snm,smk->snk', cov_imag, w_imag, precision=highest)
    prod_imag = jnp.einsum('snm,smk->snk', cov_real, w_imag, precision=highest) + jnp.einsum('snm,smk->snk', cov_imag, w_real, precision=highest)
    quadratic = lax.optimization_barrier(jnp.sum(w_real * prod_real + w_imag * prod_imag, axis=(0, 1)))
    inverse = 1.0 / jnp.sqrt(quadratic + loading)
    filtered = jnp.stack([out_real * inverse[:, None], out_imag * inverse[:, None]])
    energy = lax.optimization_barrier(jnp.sum(out_real * out_real + out_imag * out_imag, axis=1))
    covariance = jnp.concatenate([cov_real, cov_imag], axis=-1)
    return (covariance, filtered, energy)

def reference(samples, beam_weights, subarrays, training):
    factor = 1.0 / (GB * P_SIZE)

    def one_block(index):
        start = (index * GB).astype(jnp.int32)
        snaps = lax.dynamic_slice_in_dim(samples, start, GB, 2).reshape(2, C, GB * P_SIZE)
        gates_on = lax.dynamic_slice_in_dim(training, start, GB, 0).astype(jnp.float32)
        masked = jnp.repeat(gates_on, P_SIZE)
        return block_terms(snaps, subarrays[index], beam_weights[index], masked, factor)
    covs, filts, energies = lax.map(one_block, jnp.arange(NB, dtype=jnp.int32))
    filtered = filts.reshape(NB, 2, K, GB, P_SIZE).transpose(1, 2, 0, 3, 4).reshape(2, K, G, P_SIZE)
    energy = lax.optimization_barrier(jnp.sum(energies, axis=0)) / (G * P_SIZE)
    return (covs, filtered, energy)
```

```python
import functools

import jax
import jax.numpy as jnp
from jax import lax
from jax.experimental import pallas as pl
from jax.experimental.pallas import tpu as pltpu
from jax.sharding import PartitionSpec as P

F32 = jnp.float32
BF16 = jnp.bfloat16
GB = 2
NX = 8
GROUPS_RANGE_SUB = ("groups", "range", "sub")
GROUPS_RANGE = ("groups", "range")
loading = 0.05


def halves(value):
    high = value.astype(BF16)
    return high, (value - high.astype(F32)).astype(BF16)


def dot(left, right, across=False):
    dims = (((1,), (1 if across else 0,)), ((), ()))
    return lax.dot_general(left, right, dims, preferred_element_type=F32)


def dot3(left, right, across=False):
    (lh, ll), (rh, rl) = left, right
    return dot(lh, rh, across) + (dot(lh, rl, across) + dot(ll, rh, across))


def kernel(
    nz, nc, gates, x_ref, w_ref, sub_ref, train_ref,
    cov_ref, filt_ref, energy_ref,
    xv, zb, wb, sv, ev, ea, eb, mask, local_sem, send_sem, row_sem, arrived,
    w_send, w_recv, e_send, ea_sem, eb_sem,
):
    rng, core = lax.axis_index("range"), lax.axis_index("sub")
    z, x = rng // NX, rng % NX
    row = NX * nc
    rank = x * nc + core
    me = z * row + rank
    place = (z + nz - 1) % nz

    def at(z2, k):
        return {"range": z2 * NX + k // nc, "sub": k % nc}

    barrier = pltpu.get_barrier_semaphore()
    load = pltpu.make_async_copy(x_ref, xv, local_sem.at[0])
    load.start()

    def greet(i, _):
        pl.semaphore_signal(barrier, inc=1, device_id=at(z, (rank + 1 + i) % row))
        return 0

    lax.fori_loop(0, row - 1, greet, 0)

    @pl.when(place == 0)
    def _():
        pl.semaphore_wait(barrier, row - 1)

    @pl.when(place > 0)
    def _():
        pl.semaphore_wait(barrier, row)

    @pl.when(place < nz - 1)
    def _():
        pl.semaphore_signal(barrier, inc=1, device_id=at((z + 1) % nz, rank))

    def tell(i, _):
        pl.semaphore_signal(arrived.at[place], inc=1, device_id=at((z + nz - 1 - i) % nz, rank))
        return 0

    lax.fori_loop(0, place, tell, 0)
    load.wait()

    def send(z2, i, _):
        k = (rank + i) % row
        pltpu.make_async_remote_copy(
            src_ref=xv.at[:, pl.ds(gates * (z2 * row + k), gates), :],
            dst_ref=zb.at[:, pl.ds(gates * me, gates), :],
            send_sem=send_sem, recv_sem=row_sem.at[z], device_id=at(z2, k),
        ).start()
        return 0

    def send_row(z2):
        lax.fori_loop(0, row, functools.partial(send, z2), 0)

    def known(j, _):
        off = nz // 2 + lax.select(j % 2 == 0, j // 2, -(j // 2) - 1)

        @pl.when(off <= place)
        def _():
            send_row((z + nz - off) % nz)

        return 0

    lax.fori_loop(0, nz - 1, known, 0)
    lax.fori_loop(1, row, functools.partial(send, z), 0)

    def later(p, _):
        pl.semaphore_wait(arrived.at[p], 1)
        send_row((p + 1) % nz)
        return 0

    lax.fori_loop(place + 1, nz, later, 0)

    w_copy = pltpu.make_async_remote_copy(
        src_ref=w_ref.at[1 - core], dst_ref=wb.at[core], send_sem=w_send, recv_sem=w_recv,
        device_id={"sub": 1 - core},
    )
    w_copy.start()
    w_own = pltpu.make_async_copy(w_ref.at[core], wb.at[core], local_sem.at[1])
    w_own.start()
    s_own = pltpu.make_async_copy(sub_ref, sv, local_sem.at[2])
    s_own.start()
    t_own = pltpu.make_async_copy(train_ref, mask, local_sem.at[3])
    t_own.start()

    here = pl.ds(gates * me, gates)
    for plane in range(4):
        zb[plane, here, :] = xv[plane, here, :]

    s_own.wait()
    t_own.wait()
    w_own.wait()
    w_copy.wait()
    ns, _, width, half_beams = wb.shape[1:]
    beams = 2 * half_beams
    chans = ns * width
    flat = ns * 2 * width
    lane = lax.broadcasted_iota(jnp.int32, (beams, 2 * width), 1)
    first = lane < width
    wt = jnp.concatenate(
        [wb[h].reshape(flat, half_beams).T for h in range(2)], axis=0
    )
    wts = [wt[:, s * 2 * width : (s + 1) * 2 * width] for s in range(ns)]
    parts = [[], []]
    for s in range(0, ns, 2):
        a, b = wts[s], wts[s + 1]
        parts[0].append(jnp.where(first, a, pltpu.roll(b, width, 1)))
        parts[1].append(jnp.where(first, pltpu.roll(a, width, 1), b))
    wr, wi = (jnp.concatenate(p, axis=1) for p in parts)
    column = lax.broadcasted_iota(jnp.int32, (width, chans), 1)
    name = 2 * (column % (chans // 2)) + column // (chans // 2)
    eye = lax.broadcasted_iota(jnp.int32, (width, width), 0) == lax.broadcasted_iota(jnp.int32, (width, width), 1)
    rows = []
    for s in range(ns):
        line = jnp.broadcast_to(sv[s : s + 1, :].astype(F32), (width, width))
        chosen = jnp.sum(jnp.where(eye, line, 0.0), axis=1, keepdims=True)
        rows.append(jnp.where(chosen == name.astype(F32), 1.0, 0.0))
    pick = jnp.concatenate(rows, axis=0).astype(BF16)
    wr_h, wr_l = halves(wr)
    wi_h, wi_l = halves(wi)
    moved = dot(jnp.concatenate([wr_h, wr_l, wi_h, wi_l], axis=0), pick).astype(BF16)
    mr_h, mr_l, mi_h, mi_l = (moved[i * beams : (i + 1) * beams] for i in range(4))
    steer = tuple(
        jnp.concatenate([jnp.concatenate([r, i], axis=1), jnp.concatenate([-i, r], axis=1)], axis=0)
        for r, i in ((mr_h, mi_h), (mr_l, mi_l))
    )

    block = zb.at[:, pl.ds(0, gates * row), :]
    short = zb.at[:, pl.ds(0, gates * (row - 1)), :]

    def receive(z2, _):
        @pl.when(z2 == z)
        def _():
            pltpu.make_async_copy(short, short, row_sem.at[z2]).wait()

        @pl.when(z2 != z)
        def _():
            pltpu.make_async_copy(block, block, row_sem.at[z2]).wait()

        return 0

    lax.fori_loop(0, nz, receive, 0)

    peers = nz * row
    planes = [
        jnp.concatenate([zb[plane, pl.ds(g, peers, stride=gates), :] for g in range(gates)], axis=1)
        for plane in range(4)
    ]
    data = halves(jnp.concatenate(planes, axis=0))
    beam = dot3(steer, data)
    out_r, out_i = beam[:beams], beam[beams:]
    power = jnp.sum(out_r * out_r + out_i * out_i, axis=1, keepdims=True)
    eye_b = lax.broadcasted_iota(jnp.int32, (beams, beams), 0) == lax.broadcasted_iota(jnp.int32, (beams, beams), 1)
    ev[0] = jnp.sum(jnp.where(eye_b, power, 0.0), axis=0, keepdims=True)
    ea[rank] = ev[0]

    def share_row(i, _):
        pltpu.make_async_remote_copy(
            src_ref=ev.at[0], dst_ref=ea.at[rank], send_sem=e_send.at[0], recv_sem=ea_sem,
            device_id=at(z, (rank + i) % row),
        ).start()
        return 0

    lax.fori_loop(1, row, share_row, 0)

    got = [
        dot(pick, d[part * chans : (part + 1) * chans]).astype(BF16) for d in data for part in range(2)
    ]
    gate_of = lax.broadcasted_iota(jnp.int32, (2 * width, got[0].shape[1]), 1) // (got[0].shape[1] // gates)
    on = jnp.where(gate_of == 0, mask[0].astype(F32), mask[1].astype(F32)).astype(BF16)
    factor = 1.0 / got[0].shape[1]
    lane_s = lax.broadcasted_iota(jnp.int32, (width, 2 * width), 1) < width
    total = jnp.zeros((beams, 2 * width), F32)

    def subarray(s):
        cut = slice(s * width, (s + 1) * width)
        high = jnp.concatenate([got[0][cut], got[1][cut]], axis=0)
        low = jnp.concatenate([got[2][cut], got[3][cut]], axis=0)
        full = dot3((high * on, low * on), (high, low), across=True) * factor
        top, turned = full[:width], pltpu.roll(full[width:], width, 1)
        cov = turned + jnp.where(lane_s, top, -top)
        cov_ref[s] = cov
        matrix = jnp.concatenate([jnp.where(lane_s, cov, -cov), pltpu.roll(cov, width, 1)], axis=0)
        return dot3(halves(wts[s]), halves(matrix)) * wts[s]

    for s in range(ns):
        total = total + subarray(s)

    ra = ea.at[pl.ds(0, row - 1)]
    pltpu.make_async_copy(ra, ra, ea_sem).wait()
    ev[1] = jnp.sum(ea[...], axis=0)
    eb[z] = ev[1]

    def share_column(i, _):
        pltpu.make_async_remote_copy(
            src_ref=ev.at[1], dst_ref=eb.at[z], send_sem=e_send.at[1], recv_sem=eb_sem,
            device_id=at((z + i) % nz, rank),
        ).start()
        return 0

    lax.fori_loop(1, nz, share_column, 0)

    inverse = 1.0 / jnp.sqrt(jnp.sum(total, axis=1, keepdims=True) + loading)
    pulses = out_r.shape[1] // gates
    for part, out in enumerate((out_r, out_i)):
        scaled = out * inverse
        for g in range(gates):
            filt_ref[part, pl.ds(g, beams, stride=gates), :] = scaled[:, g * pulses : (g + 1) * pulses]

    every = zb.at[:, pl.ds(0, gates * (peers - 1)), :]
    pltpu.make_async_copy(every, every, send_sem).wait()
    pltpu.make_async_copy(ra, ra, e_send.at[0]).wait()
    rb = eb.at[pl.ds(0, nz - 1)]
    pltpu.make_async_copy(rb, rb, e_send.at[1]).wait()
    pltpu.make_async_copy(rb, rb, eb_sem).wait()
    energy_ref[...] = jnp.sum(eb[...], axis=0) * (1.0 / (peers * gates * pulses))


def body(samples, beam_weights, subarrays, training):
    range_count, nc = lax.axis_size("range"), lax.axis_size("sub")
    nz = range_count // NX
    parts_iq, chan_dev, all_gates, pulses = samples.shape
    gates = training.shape[0]
    _, ns, _, width, half_beams = beam_weights.shape
    beams = half_beams * nc
    anywhere = pl.BlockSpec(memory_space=pl.ANY)
    vmem = pl.BlockSpec(memory_space=pltpu.VMEM)
    dma, regular = pltpu.SemaphoreType.DMA, pltpu.SemaphoreType.REGULAR
    cov, filt, energy = pl.pallas_call(
        functools.partial(kernel, nz, nc, gates),
        out_shape=(
            jax.ShapeDtypeStruct((ns, width, 2 * width), F32),
            jax.ShapeDtypeStruct((parts_iq, beams * gates, pulses), F32),
            jax.ShapeDtypeStruct((1, beams), F32),
        ),
        in_specs=[anywhere] * 4,
        out_specs=(vmem, vmem, vmem),
        scratch_shapes=[
            pltpu.VMEM((parts_iq * chan_dev, all_gates, pulses), F32),
            pltpu.VMEM((parts_iq * chan_dev, all_gates, pulses), F32),
            pltpu.VMEM((nc, ns, 2, width, half_beams), F32),
            pltpu.VMEM((ns, width), jnp.int32),
            pltpu.VMEM((2, 1, beams), F32),
            pltpu.VMEM((NX * nc, 1, beams), F32),
            pltpu.VMEM((nz, 1, beams), F32),
            pltpu.SMEM((gates,), jnp.int32),
            dma((4,)),
            dma,
            dma((nz,)),
            regular((nz,)),
            dma,
            dma,
            dma((2,)),
            dma,
            dma,
        ],
        compiler_params=pltpu.CompilerParams(collective_id=1, has_side_effects=True),
    )(
        samples.reshape(parts_iq * chan_dev, all_gates, pulses),
        beam_weights,
        subarrays.reshape(ns, width),
        training,
    )
    return (
        cov.reshape(1, ns, width, 2 * width),
        filt.reshape(parts_iq, beams, gates, pulses),
        energy.reshape(beams),
    )


def solution(mesh):
    return jax.shard_map(
        body,
        mesh=mesh,
        in_specs=(
            P(None, GROUPS_RANGE_SUB, None, None),
            P(GROUPS_RANGE, None, None, None, "sub"),
            P(GROUPS_RANGE_SUB, None, None),
            P(GROUPS_RANGE_SUB),
        ),
        out_specs=(
            P(GROUPS_RANGE_SUB, None, None, None),
            P(None, None, GROUPS_RANGE_SUB, None),
            P("groups"),
        ),
        check_vma=False,
    )
```

```python
import functools

import jax
import jax.numpy as jnp
from jax import lax
from jax.experimental import pallas as pl
from jax.experimental.pallas import tpu as pltpu
from jax.sharding import PartitionSpec as P

F32 = jnp.float32
BF16 = jnp.bfloat16
GROUP = 4
NX = 8
GROUPS_RANGE_SUB = ("groups", "range", "sub")
GROUPS_RANGE = ("groups", "range")
loading = 0.05


def halves(value):
    high = value.astype(BF16)
    return high, (value - high.astype(F32)).astype(BF16)


def dot(left, right, across=False):
    dims = (((1,), (1 if across else 0,)), ((), ()))
    return lax.dot_general(left, right, dims, preferred_element_type=F32)


def dot3(left, right, across=False):
    (lh, ll), (rh, rl) = left, right
    return dot(lh, rh, across) + (dot(lh, rl, across) + dot(ll, rh, across))


def kernel(
    nz, nc, gates, x_ref, w_ref, sub_ref, train_ref,
    cov_ref, filt_ref, energy_ref,
    xv, zb, wb, steer, data, sv, ev, ea, eb, mask, local_sem, send_sem, row_sem, arrived,
    w_send, w_recv, e_send, ea_sem, eb_sem,
):
    rng, core = lax.axis_index("range"), lax.axis_index("sub")
    z, x = rng // NX, rng % NX
    row = NX * nc
    rank = x * nc + core
    me = z * row + rank
    place = (z + nz - 1) % nz

    def at(z2, k):
        return {"range": z2 * NX + k // nc, "sub": k % nc}

    def outward(j, count):
        return count // 2 + lax.select(j % 2 == 0, j // 2, -(j // 2) - 1)

    barrier = pltpu.get_barrier_semaphore()
    load = pltpu.make_async_copy(x_ref, xv, local_sem.at[0])
    load.start()

    def greet(j, _):
        pl.semaphore_signal(barrier, inc=1, device_id=at(z, (rank + outward(j, row)) % row))
        return 0

    lax.fori_loop(0, row - 1, greet, 0)

    @pl.when(place == 0)
    def _():
        pl.semaphore_wait(barrier, row - 1)

    @pl.when(place > 0)
    def _():
        pl.semaphore_wait(barrier, row)

    @pl.when(place < nz - 1)
    def _():
        pl.semaphore_signal(barrier, inc=1, device_id=at((z + 1) % nz, rank))

    def tell(i, _):
        pl.semaphore_signal(arrived.at[place], inc=1, device_id=at((z + nz - 1 - i) % nz, rank))
        return 0

    lax.fori_loop(0, place, tell, 0)
    load.wait()

    def send(z2, i, _):
        k = (rank + i) % row
        pltpu.make_async_remote_copy(
            src_ref=xv.at[:, pl.ds(gates * (z2 * row + k), gates), :],
            dst_ref=zb.at[:, pl.ds(gates * me, gates), :],
            send_sem=send_sem, recv_sem=row_sem.at[z], device_id=at(z2, k),
        ).start()
        return 0

    def send_row(z2):
        lax.fori_loop(0, row, functools.partial(send, z2), 0)

    def known(j, _):
        off = outward(j, nz)

        @pl.when(off <= place)
        def _():
            send_row((z + nz - off) % nz)

        return 0

    lax.fori_loop(0, nz - 1, known, 0)
    lax.fori_loop(1, row, functools.partial(send, z), 0)

    def later(p, _):
        pl.semaphore_wait(arrived.at[p], 1)
        send_row((p + 1) % nz)
        return 0

    lax.fori_loop(place + 1, nz, later, 0)

    w_copy = pltpu.make_async_remote_copy(
        src_ref=w_ref.at[1 - core], dst_ref=wb.at[core], send_sem=w_send, recv_sem=w_recv,
        device_id={"sub": 1 - core},
    )
    w_copy.start()
    w_own = pltpu.make_async_copy(w_ref.at[core], wb.at[core], local_sem.at[1])
    w_own.start()
    s_own = pltpu.make_async_copy(sub_ref, sv, local_sem.at[2])
    s_own.start()
    t_own = pltpu.make_async_copy(train_ref, mask, local_sem.at[3])
    t_own.start()

    here = pl.ds(gates * me, gates)
    for plane in range(4):
        zb[plane, here, :] = xv[plane, here, :]

    s_own.wait()
    t_own.wait()
    w_own.wait()
    w_copy.wait()
    ns, _, width, half_beams = wb.shape[1:]
    beams = 2 * half_beams
    chans = ns * width
    flat = ns * 2 * width
    lane = lax.broadcasted_iota(jnp.int32, (beams, 2 * width), 1)
    first = lane < width
    wt = jnp.concatenate(
        [wb[h].reshape(flat, half_beams).T for h in range(2)], axis=0
    )
    wts = [wt[:, s * 2 * width : (s + 1) * 2 * width] for s in range(ns)]
    parts = [[], []]
    for s in range(0, ns, 2):
        a, b = wts[s], wts[s + 1]
        parts[0].append(jnp.where(first, a, pltpu.roll(b, width, 1)))
        parts[1].append(jnp.where(first, pltpu.roll(a, width, 1), b))
    wr, wi = (jnp.concatenate(p, axis=1) for p in parts)
    column = lax.broadcasted_iota(jnp.int32, (width, chans), 1)
    span = gates * row * GROUP // 2
    name = 2 * (column // (2 * span) * span + column % span) + column // span % 2
    eye = lax.broadcasted_iota(jnp.int32, (width, width), 0) == lax.broadcasted_iota(jnp.int32, (width, width), 1)
    rows = []
    for s in range(ns):
        line = jnp.broadcast_to(sv[s : s + 1, :].astype(F32), (width, width))
        chosen = jnp.sum(jnp.where(eye, line, 0.0), axis=1, keepdims=True)
        rows.append(jnp.where(chosen == name.astype(F32), 1.0, 0.0))
    pick = jnp.concatenate(rows, axis=0).astype(BF16)
    wr_h, wr_l = halves(wr)
    wi_h, wi_l = halves(wi)
    moved = dot(jnp.concatenate([wr_h, wr_l, wi_h, wi_l], axis=0), pick).astype(BF16)
    mr_h, mr_l, mi_h, mi_l = (moved[i * beams : (i + 1) * beams] for i in range(4))
    for q in range(nz // GROUP):
        cut = slice(q * 2 * span, (q + 1) * 2 * span)
        for half, (r, i) in enumerate(((mr_h[:, cut], mi_h[:, cut]), (mr_l[:, cut], mi_l[:, cut]))):
            steer[half, q] = jnp.concatenate(
                [jnp.concatenate([r, i], axis=1), jnp.concatenate([-i, r], axis=1)], axis=0
            )

    block = zb.at[:, pl.ds(0, gates * row), :]
    short = zb.at[:, pl.ds(0, gates * (row - 1)), :]

    def receive(z2, _):
        @pl.when(z2 == z)
        def _():
            pltpu.make_async_copy(short, short, row_sem.at[z2]).wait()

        @pl.when(z2 != z)
        def _():
            pltpu.make_async_copy(block, block, row_sem.at[z2]).wait()

        return 0

    peers = nz * row
    beam = None
    for q in (*range(1, nz // GROUP), 0):
        lax.fori_loop(q * GROUP, (q + 1) * GROUP, receive, 0)
        planes = [
            jnp.concatenate(
                [zb[plane, pl.ds(gates * q * span + g, span, stride=gates), :] for g in range(gates)], axis=1
            )
            for plane in range(4)
        ]
        data[0, q], data[1, q] = halves(jnp.concatenate(planes, axis=0))
        term = dot3((steer[0, q], steer[1, q]), (data[0, q], data[1, q]))
        beam = term if beam is None else beam + term
    out_r, out_i = beam[:beams], beam[beams:]
    power = jnp.sum(out_r * out_r + out_i * out_i, axis=1, keepdims=True)
    eye_b = lax.broadcasted_iota(jnp.int32, (beams, beams), 0) == lax.broadcasted_iota(jnp.int32, (beams, beams), 1)
    ev[0] = jnp.sum(jnp.where(eye_b, power, 0.0), axis=0, keepdims=True)
    ea[rank] = ev[0]

    def share_row(i, _):
        pltpu.make_async_remote_copy(
            src_ref=ev.at[0], dst_ref=ea.at[rank], send_sem=e_send.at[0], recv_sem=ea_sem,
            device_id=at(z, (rank + i) % row),
        ).start()
        return 0

    lax.fori_loop(1, row, share_row, 0)

    got = [
        dot(
            pick,
            jnp.concatenate(
                [data[half, q, pl.ds(part * 2 * span, 2 * span), :] for q in range(nz // GROUP)], axis=0
            ),
        ).astype(BF16)
        for half in range(2)
        for part in range(2)
    ]
    gate_of = lax.broadcasted_iota(jnp.int32, (2 * width, got[0].shape[1]), 1) // (got[0].shape[1] // gates)
    on = jnp.where(gate_of == 0, mask[0].astype(F32), mask[1].astype(F32)).astype(BF16)
    factor = 1.0 / got[0].shape[1]
    lane_s = lax.broadcasted_iota(jnp.int32, (width, 2 * width), 1) < width
    total = jnp.zeros((beams, 2 * width), F32)

    def subarray(s):
        cut = slice(s * width, (s + 1) * width)
        high = jnp.concatenate([got[0][cut], got[1][cut]], axis=0)
        low = jnp.concatenate([got[2][cut], got[3][cut]], axis=0)
        full = dot3((high * on, low * on), (high, low), across=True) * factor
        top, turned = full[:width], pltpu.roll(full[width:], width, 1)
        cov = turned + jnp.where(lane_s, top, -top)
        cov_ref[s] = cov
        matrix = jnp.concatenate([jnp.where(lane_s, cov, -cov), pltpu.roll(cov, width, 1)], axis=0)
        return dot3(halves(wts[s]), halves(matrix)) * wts[s]

    for s in range(ns):
        total = total + subarray(s)

    ra = ea.at[pl.ds(0, row - 1)]
    pltpu.make_async_copy(ra, ra, ea_sem).wait()
    ev[1] = jnp.sum(ea[...], axis=0)
    eb[z] = ev[1]

    def share_column(i, _):
        pltpu.make_async_remote_copy(
            src_ref=ev.at[1], dst_ref=eb.at[z], send_sem=e_send.at[1], recv_sem=eb_sem,
            device_id=at((z + i) % nz, rank),
        ).start()
        return 0

    lax.fori_loop(1, nz, share_column, 0)

    inverse = 1.0 / jnp.sqrt(jnp.sum(total, axis=1, keepdims=True) + loading)
    pulses = out_r.shape[1] // gates
    for part, out in enumerate((out_r, out_i)):
        scaled = out * inverse
        for g in range(gates):
            filt_ref[part, pl.ds(g, beams, stride=gates), :] = scaled[:, g * pulses : (g + 1) * pulses]

    every = zb.at[:, pl.ds(0, gates * (peers - 1)), :]
    pltpu.make_async_copy(every, every, send_sem).wait()
    pltpu.make_async_copy(ra, ra, e_send.at[0]).wait()
    rb = eb.at[pl.ds(0, nz - 1)]
    pltpu.make_async_copy(rb, rb, e_send.at[1]).wait()
    pltpu.make_async_copy(rb, rb, eb_sem).wait()
    energy_ref[...] = jnp.sum(eb[...], axis=0) * (1.0 / (peers * gates * pulses))


def writer(*refs):
    sem = refs[-1]
    copies = [pltpu.make_async_copy(refs[i], refs[i + 3], sem.at[i]) for i in range(3)]
    for copy in copies:
        copy.start()
    for copy in copies:
        copy.wait()


def body(samples, beam_weights, subarrays, training):
    range_count, nc = lax.axis_size("range"), lax.axis_size("sub")
    nz = range_count // NX
    parts_iq, chan_dev, all_gates, pulses = samples.shape
    gates = training.shape[0]
    _, ns, _, width, half_beams = beam_weights.shape
    beams = half_beams * nc
    anywhere = pl.BlockSpec(memory_space=pl.ANY)
    vmem = pl.BlockSpec(memory_space=pltpu.VMEM)
    dma, regular = pltpu.SemaphoreType.DMA, pltpu.SemaphoreType.REGULAR
    cov, filt, energy = pl.pallas_call(
        functools.partial(kernel, nz, nc, gates),
        out_shape=(
            pltpu.VMEM((ns, width, 2 * width), F32),
            pltpu.VMEM((parts_iq, beams * gates, pulses), F32),
            pltpu.VMEM((1, beams), F32),
        ),
        in_specs=[anywhere] * 4,
        out_specs=(vmem, vmem, vmem),
        scratch_shapes=[
            pltpu.VMEM((parts_iq * chan_dev, all_gates, pulses), F32),
            pltpu.VMEM((parts_iq * chan_dev, all_gates, pulses), F32),
            pltpu.VMEM((nc, ns, 2, width, half_beams), F32),
            pltpu.VMEM((2, nz // GROUP, 2 * beams, 4 * NX * nc * GROUP), BF16),
            pltpu.VMEM((2, nz // GROUP, 4 * NX * nc * GROUP, gates * pulses), BF16),
            pltpu.VMEM((ns, width), jnp.int32),
            pltpu.VMEM((2, 1, beams), F32),
            pltpu.VMEM((NX * nc, 1, beams), F32),
            pltpu.VMEM((nz, 1, beams), F32),
            pltpu.SMEM((gates,), jnp.int32),
            dma((4,)),
            dma,
            dma((nz,)),
            regular((nz,)),
            dma,
            dma,
            dma((2,)),
            dma,
            dma,
        ],
        compiler_params=pltpu.CompilerParams(collective_id=1, has_side_effects=True),
    )(
        samples.reshape(parts_iq * chan_dev, all_gates, pulses),
        beam_weights,
        subarrays.reshape(ns, width),
        training,
    )
    results = tuple(pltpu.with_memory_space_constraint(r, pltpu.VMEM) for r in (cov, filt, energy))
    cov, filt, energy = pl.pallas_call(
        writer,
        out_shape=tuple(jax.ShapeDtypeStruct(r.shape, F32) for r in results),
        in_specs=[vmem] * 3,
        out_specs=(anywhere,) * 3,
        scratch_shapes=[dma((3,))],
    )(*results)
    return (
        cov.reshape(1, ns, width, 2 * width),
        filt.reshape(parts_iq, beams, gates, pulses),
        energy.reshape(beams),
    )


def solution(mesh):
    return jax.shard_map(
        body,
        mesh=mesh,
        in_specs=(
            P(None, GROUPS_RANGE_SUB, None, None),
            P(GROUPS_RANGE, None, None, None, "sub"),
            P(GROUPS_RANGE_SUB, None, None),
            P(GROUPS_RANGE_SUB),
        ),
        out_specs=(
            P(GROUPS_RANGE_SUB, None, None, None),
            P(None, None, GROUPS_RANGE_SUB, None),
            P("groups"),
        ),
        check_vma=False,
    )
```

```python
import functools

import jax
import jax.numpy as jnp
from jax import lax
from jax.experimental import pallas as pl
from jax.experimental.pallas import tpu as pltpu
from jax.sharding import PartitionSpec as P

F32 = jnp.float32
BF16 = jnp.bfloat16
GROUP = 4
NX = 8
GROUPS_RANGE_SUB = ("groups", "range", "sub")
GROUPS_RANGE = ("groups", "range")
loading = 0.05


def halves(value):
    high = value.astype(BF16)
    return high, (value - high.astype(F32)).astype(BF16)


def dot(left, right, across=False):
    dims = (((1,), (1 if across else 0,)), ((), ()))
    return lax.dot_general(left, right, dims, preferred_element_type=F32)


def dot3(left, right, across=False):
    (lh, ll), (rh, rl) = left, right
    return dot(lh, rh, across) + (dot(lh, rl, across) + dot(ll, rh, across))


def kernel(
    nz, nc, gates, x_ref, w_ref, sub_ref, train_ref,
    cov_ref, filt_ref, energy_ref,
    xv, zb, wb, steer, data, sv, ev, ea, eb, mask, local_sem, send_sem, row_sem, arrived,
    w_send, w_recv, e_send, ea_sem, eb_sem,
):
    rng, core = lax.axis_index("range"), lax.axis_index("sub")
    z, x = rng // NX, rng % NX
    row = NX * nc
    rank = x * nc + core
    me = z * row + rank
    place = (z + nz - 1) % nz

    def at(z2, k):
        return {"range": z2 * NX + k // nc, "sub": k % nc}

    def outward(j, count):
        return count // 2 + lax.select(j % 2 == 0, j // 2, -(j // 2) - 1)

    barrier = pltpu.get_barrier_semaphore()
    load = pltpu.make_async_copy(x_ref, xv, local_sem.at[0])
    load.start()

    def greet(j, _):
        pl.semaphore_signal(barrier, inc=1, device_id=at(z, (rank + outward(j, row)) % row))
        return 0

    lax.fori_loop(0, row - 1, greet, 0)

    @pl.when(place == 0)
    def _():
        pl.semaphore_wait(barrier, row - 1)

    @pl.when(place > 0)
    def _():
        pl.semaphore_wait(barrier, row)

    @pl.when(place < nz - 1)
    def _():
        pl.semaphore_signal(barrier, inc=1, device_id=at((z + 1) % nz, rank))

    def tell(i, _):
        pl.semaphore_signal(arrived.at[place], inc=1, device_id=at((z + nz - 1 - i) % nz, rank))
        return 0

    lax.fori_loop(0, place, tell, 0)
    load.wait()

    def send(z2, i, _):
        k = (rank + i) % row
        pltpu.make_async_remote_copy(
            src_ref=xv.at[:, pl.ds(gates * (z2 * row + k), gates), :],
            dst_ref=zb.at[:, pl.ds(gates * me, gates), :],
            send_sem=send_sem, recv_sem=row_sem.at[z], device_id=at(z2, k),
        ).start()
        return 0

    def send_row(z2):
        lax.fori_loop(0, row, functools.partial(send, z2), 0, unroll=row)

    def known(j, _):
        off = outward(j, nz)

        @pl.when(off <= place)
        def _():
            send_row((z + nz - off) % nz)

        return 0

    lax.fori_loop(0, nz - 1, known, 0)
    lax.fori_loop(1, row, functools.partial(send, z), 0)

    def later(p, _):
        pl.semaphore_wait(arrived.at[p], 1)
        send_row((p + 1) % nz)
        return 0

    lax.fori_loop(place + 1, nz, later, 0)

    w_copy = pltpu.make_async_remote_copy(
        src_ref=w_ref.at[1 - core], dst_ref=wb.at[core], send_sem=w_send, recv_sem=w_recv,
        device_id={"sub": 1 - core},
    )
    w_copy.start()
    w_own = pltpu.make_async_copy(w_ref.at[core], wb.at[core], local_sem.at[1])
    w_own.start()
    s_own = pltpu.make_async_copy(sub_ref, sv, local_sem.at[2])
    s_own.start()
    t_own = pltpu.make_async_copy(train_ref, mask, local_sem.at[3])
    t_own.start()

    here = pl.ds(gates * me, gates)
    for plane in range(4):
        zb[plane, here, :] = xv[plane, here, :]

    s_own.wait()
    t_own.wait()
    w_own.wait()
    w_copy.wait()
    ns, _, width, half_beams = wb.shape[1:]
    beams = 2 * half_beams
    chans = ns * width
    flat = ns * 2 * width
    lane = lax.broadcasted_iota(jnp.int32, (beams, 2 * width), 1)
    first = lane < width
    wt = jnp.concatenate(
        [wb[h].reshape(flat, half_beams).T for h in range(2)], axis=0
    )
    wts = [wt[:, s * 2 * width : (s + 1) * 2 * width] for s in range(ns)]
    parts = [[], []]
    for s in range(0, ns, 2):
        a, b = wts[s], wts[s + 1]
        parts[0].append(jnp.where(first, a, pltpu.roll(b, width, 1)))
        parts[1].append(jnp.where(first, pltpu.roll(a, width, 1), b))
    wr, wi = (jnp.concatenate(p, axis=1) for p in parts)
    column = lax.broadcasted_iota(jnp.int32, (width, chans), 1)
    span = gates * row * GROUP // 2
    name = 2 * (column // (2 * span) * span + column % span) + column // span % 2
    eye = lax.broadcasted_iota(jnp.int32, (width, width), 0) == lax.broadcasted_iota(jnp.int32, (width, width), 1)
    rows = []
    for s in range(ns):
        line = jnp.broadcast_to(sv[s : s + 1, :].astype(F32), (width, width))
        chosen = jnp.sum(jnp.where(eye, line, 0.0), axis=1, keepdims=True)
        rows.append(jnp.where(chosen == name.astype(F32), 1.0, 0.0))
    pick = jnp.concatenate(rows, axis=0).astype(BF16)
    wr_h, wr_l = halves(wr)
    wi_h, wi_l = halves(wi)
    moved = dot(jnp.concatenate([wr_h, wr_l, wi_h, wi_l], axis=0), pick).astype(BF16)
    mr_h, mr_l, mi_h, mi_l = (moved[i * beams : (i + 1) * beams] for i in range(4))
    for q in range(nz // GROUP):
        cut = slice(q * 2 * span, (q + 1) * 2 * span)
        for half, (r, i) in enumerate(((mr_h[:, cut], mi_h[:, cut]), (mr_l[:, cut], mi_l[:, cut]))):
            steer[half, q] = jnp.concatenate(
                [jnp.concatenate([r, i], axis=1), jnp.concatenate([-i, r], axis=1)], axis=0
            )

    block = zb.at[:, pl.ds(0, gates * row), :]
    short = zb.at[:, pl.ds(0, gates * (row - 1)), :]

    def receive(z2, _):
        @pl.when(z2 == z)
        def _():
            pltpu.make_async_copy(short, short, row_sem.at[z2]).wait()

        @pl.when(z2 != z)
        def _():
            pltpu.make_async_copy(block, block, row_sem.at[z2]).wait()

        return 0

    peers = nz * row
    beam = None
    for q in (*range(1, nz // GROUP), 0):
        lax.fori_loop(q * GROUP, (q + 1) * GROUP, receive, 0)
        planes = [
            jnp.concatenate(
                [zb[plane, pl.ds(gates * q * span + g, span, stride=gates), :] for g in range(gates)], axis=1
            )
            for plane in range(4)
        ]
        data[0, q], data[1, q] = halves(jnp.concatenate(planes, axis=0))
        term = dot3((steer[0, q], steer[1, q]), (data[0, q], data[1, q]))
        beam = term if beam is None else beam + term
    out_r, out_i = beam[:beams], beam[beams:]
    power = jnp.sum(out_r * out_r + out_i * out_i, axis=1, keepdims=True)
    eye_b = lax.broadcasted_iota(jnp.int32, (beams, beams), 0) == lax.broadcasted_iota(jnp.int32, (beams, beams), 1)
    ev[0] = jnp.sum(jnp.where(eye_b, power, 0.0), axis=0, keepdims=True)
    ea[rank] = ev[0]

    def share_row(i, _):
        pltpu.make_async_remote_copy(
            src_ref=ev.at[0], dst_ref=ea.at[rank], send_sem=e_send.at[0], recv_sem=ea_sem,
            device_id=at(z, (rank + i) % row),
        ).start()
        return 0

    lax.fori_loop(1, row, share_row, 0)

    got = [
        dot(
            pick,
            jnp.concatenate(
                [data[half, q, pl.ds(part * 2 * span, 2 * span), :] for q in range(nz // GROUP)], axis=0
            ),
        ).astype(BF16)
        for half in range(2)
        for part in range(2)
    ]
    gate_of = lax.broadcasted_iota(jnp.int32, (2 * width, got[0].shape[1]), 1) // (got[0].shape[1] // gates)
    on = jnp.where(gate_of == 0, mask[0].astype(F32), mask[1].astype(F32)).astype(BF16)
    factor = 1.0 / got[0].shape[1]
    lane_s = lax.broadcasted_iota(jnp.int32, (width, 2 * width), 1) < width
    total = jnp.zeros((beams, 2 * width), F32)

    def subarray(s):
        cut = slice(s * width, (s + 1) * width)
        high = jnp.concatenate([got[0][cut], got[1][cut]], axis=0)
        low = jnp.concatenate([got[2][cut], got[3][cut]], axis=0)
        full = dot3((high * on, low * on), (high, low), across=True) * factor
        top, turned = full[:width], pltpu.roll(full[width:], width, 1)
        cov = turned + jnp.where(lane_s, top, -top)
        cov_ref[s] = cov
        matrix = jnp.concatenate([jnp.where(lane_s, cov, -cov), pltpu.roll(cov, width, 1)], axis=0)
        return dot3(halves(wts[s]), halves(matrix)) * wts[s]

    for s in range(ns):
        total = total + subarray(s)

    ra = ea.at[pl.ds(0, row - 1)]
    pltpu.make_async_copy(ra, ra, ea_sem).wait()
    ev[1] = jnp.sum(ea[...], axis=0)
    eb[z] = ev[1]

    def share_column(i, _):
        pltpu.make_async_remote_copy(
            src_ref=ev.at[1], dst_ref=eb.at[z], send_sem=e_send.at[1], recv_sem=eb_sem,
            device_id=at((z + i) % nz, rank),
        ).start()
        return 0

    lax.fori_loop(1, nz, share_column, 0)

    inverse = 1.0 / jnp.sqrt(jnp.sum(total, axis=1, keepdims=True) + loading)
    pulses = out_r.shape[1] // gates
    for part, out in enumerate((out_r, out_i)):
        scaled = out * inverse
        for g in range(gates):
            filt_ref[part, pl.ds(g, beams, stride=gates), :] = scaled[:, g * pulses : (g + 1) * pulses]

    every = zb.at[:, pl.ds(0, gates * (peers - 1)), :]
    pltpu.make_async_copy(every, every, send_sem).wait()
    pltpu.make_async_copy(ra, ra, e_send.at[0]).wait()
    rb = eb.at[pl.ds(0, nz - 1)]
    pltpu.make_async_copy(rb, rb, e_send.at[1]).wait()
    pltpu.make_async_copy(rb, rb, eb_sem).wait()
    energy_ref[...] = jnp.sum(eb[...], axis=0) * (1.0 / (peers * gates * pulses))


def writer(*refs):
    sem = refs[-1]
    copies = [pltpu.make_async_copy(refs[i], refs[i + 3], sem.at[i]) for i in range(3)]
    for copy in copies:
        copy.start()
    for copy in copies:
        copy.wait()


def body(samples, beam_weights, subarrays, training):
    range_count, nc = lax.axis_size("range"), lax.axis_size("sub")
    nz = range_count // NX
    parts_iq, chan_dev, all_gates, pulses = samples.shape
    gates = training.shape[0]
    _, ns, _, width, half_beams = beam_weights.shape
    beams = half_beams * nc
    anywhere = pl.BlockSpec(memory_space=pl.ANY)
    vmem = pl.BlockSpec(memory_space=pltpu.VMEM)
    dma, regular = pltpu.SemaphoreType.DMA, pltpu.SemaphoreType.REGULAR
    cov, filt, energy = pl.pallas_call(
        functools.partial(kernel, nz, nc, gates),
        out_shape=(
            pltpu.VMEM((ns, width, 2 * width), F32),
            pltpu.VMEM((parts_iq, beams * gates, pulses), F32),
            pltpu.VMEM((1, beams), F32),
        ),
        in_specs=[anywhere] * 4,
        out_specs=(vmem, vmem, vmem),
        scratch_shapes=[
            pltpu.VMEM((parts_iq * chan_dev, all_gates, pulses), F32),
            pltpu.VMEM((parts_iq * chan_dev, all_gates, pulses), F32),
            pltpu.VMEM((nc, ns, 2, width, half_beams), F32),
            pltpu.VMEM((2, nz // GROUP, 2 * beams, 4 * NX * nc * GROUP), BF16),
            pltpu.VMEM((2, nz // GROUP, 4 * NX * nc * GROUP, gates * pulses), BF16),
            pltpu.VMEM((ns, width), jnp.int32),
            pltpu.VMEM((2, 1, beams), F32),
            pltpu.VMEM((NX * nc, 1, beams), F32),
            pltpu.VMEM((nz, 1, beams), F32),
            pltpu.SMEM((gates,), jnp.int32),
            dma((4,)),
            dma,
            dma((nz,)),
            regular((nz,)),
            dma,
            dma,
            dma((2,)),
            dma,
            dma,
        ],
        compiler_params=pltpu.CompilerParams(collective_id=1, has_side_effects=True),
    )(
        samples.reshape(parts_iq * chan_dev, all_gates, pulses),
        beam_weights,
        subarrays.reshape(ns, width),
        training,
    )
    results = tuple(pltpu.with_memory_space_constraint(r, pltpu.VMEM) for r in (cov, filt, energy))
    cov, filt, energy = pl.pallas_call(
        writer,
        out_shape=tuple(jax.ShapeDtypeStruct(r.shape, F32) for r in results),
        in_specs=[vmem] * 3,
        out_specs=(anywhere,) * 3,
        scratch_shapes=[dma((3,))],
    )(*results)
    return (
        cov.reshape(1, ns, width, 2 * width),
        filt.reshape(parts_iq, beams, gates, pulses),
        energy.reshape(beams),
    )


def solution(mesh):
    return jax.shard_map(
        body,
        mesh=mesh,
        in_specs=(
            P(None, GROUPS_RANGE_SUB, None, None),
            P(GROUPS_RANGE, None, None, None, "sub"),
            P(GROUPS_RANGE_SUB, None, None),
            P(GROUPS_RANGE_SUB),
        ),
        out_specs=(
            P(GROUPS_RANGE_SUB, None, None, None),
            P(None, None, GROUPS_RANGE_SUB, None),
            P("groups"),
        ),
        check_vma=False,
    )
```

```python
import functools

import jax
import jax.numpy as jnp
from jax import lax
from jax.experimental import pallas as pl
from jax.experimental.pallas import tpu as pltpu
from jax.sharding import PartitionSpec as P

F32 = jnp.float32
BF16 = jnp.bfloat16
GROUP = 4
NX = 8
GROUPS_RANGE_SUB = ("groups", "range", "sub")
GROUPS_RANGE = ("groups", "range")
loading = 0.05


def halves(value):
    high = value.astype(BF16)
    return high, (value - high.astype(F32)).astype(BF16)


def dot(left, right, across=False):
    dims = (((1,), (1 if across else 0,)), ((), ()))
    return lax.dot_general(left, right, dims, preferred_element_type=F32)


def dot3(left, right, across=False):
    (lh, ll), (rh, rl) = left, right
    return dot(lh, rh, across) + (dot(lh, rl, across) + dot(ll, rh, across))


def kernel(
    nz, nc, gates, x_ref, w_ref, sub_ref, train_ref,
    cov_ref, filt_ref, energy_ref,
    xv, zb, wb, steer, data, sv, ev, ea, eb, mask, local_sem, send_sem, row_sem, arrived,
    w_send, w_recv, e_send, ea_sem, eb_sem,
):
    rng, core = lax.axis_index("range"), lax.axis_index("sub")
    z, x = rng // NX, rng % NX
    row = NX * nc
    rank = x * nc + core
    me = z * row + rank
    place = (z + nz - 1) % nz

    def at(z2, k):
        return {"range": z2 * NX + k // nc, "sub": k % nc}

    def outward(j, count):
        return count // 2 + lax.select(j % 2 == 0, j // 2, -(j // 2) - 1)

    barrier = pltpu.get_barrier_semaphore()
    load = pltpu.make_async_copy(x_ref, xv, local_sem.at[0])
    load.start()

    def greet(j, _):
        pl.semaphore_signal(barrier, inc=1, device_id=at(z, (rank + outward(j, row)) % row))
        return 0

    lax.fori_loop(0, row - 1, greet, 0, unroll=row - 1)

    @pl.when(place == 0)
    def _():
        pl.semaphore_wait(barrier, row - 1)

    @pl.when(place > 0)
    def _():
        pl.semaphore_wait(barrier, row)

    @pl.when(place < nz - 1)
    def _():
        pl.semaphore_signal(barrier, inc=1, device_id=at((z + 1) % nz, rank))

    def tell(i, _):
        pl.semaphore_signal(arrived.at[place], inc=1, device_id=at((z + nz - 1 - i) % nz, rank))
        return 0

    lax.fori_loop(0, place, tell, 0)
    load.wait()

    def send(z2, i, _):
        k = (rank + i) % row
        pltpu.make_async_remote_copy(
            src_ref=xv.at[:, pl.ds(gates * (z2 * row + k), gates), :],
            dst_ref=zb.at[:, pl.ds(gates * me, gates), :],
            send_sem=send_sem, recv_sem=row_sem.at[z], device_id=at(z2, k),
        ).start()
        return 0

    def send_row(z2):
        lax.fori_loop(0, row, functools.partial(send, z2), 0, unroll=row)

    def known(j, _):
        off = outward(j, nz)

        @pl.when(off <= place)
        def _():
            send_row((z + nz - off) % nz)

        return 0

    lax.fori_loop(0, nz - 1, known, 0)
    lax.fori_loop(1, row, functools.partial(send, z), 0)

    def later(p, _):
        pl.semaphore_wait(arrived.at[p], 1)
        send_row((p + 1) % nz)
        return 0

    lax.fori_loop(place + 1, nz, later, 0)

    w_copy = pltpu.make_async_remote_copy(
        src_ref=w_ref.at[1 - core], dst_ref=wb.at[core], send_sem=w_send, recv_sem=w_recv,
        device_id={"sub": 1 - core},
    )
    w_copy.start()
    w_own = pltpu.make_async_copy(w_ref.at[core], wb.at[core], local_sem.at[1])
    w_own.start()
    s_own = pltpu.make_async_copy(sub_ref, sv, local_sem.at[2])
    s_own.start()
    t_own = pltpu.make_async_copy(train_ref, mask, local_sem.at[3])
    t_own.start()

    here = pl.ds(gates * me, gates)
    for plane in range(4):
        zb[plane, here, :] = xv[plane, here, :]

    s_own.wait()
    t_own.wait()
    w_own.wait()
    w_copy.wait()
    ns, _, width, half_beams = wb.shape[1:]
    beams = 2 * half_beams
    chans = ns * width
    flat = ns * 2 * width
    lane = lax.broadcasted_iota(jnp.int32, (beams, 2 * width), 1)
    first = lane < width
    wt = jnp.concatenate(
        [wb[h].reshape(flat, half_beams).T for h in range(2)], axis=0
    )
    wts = [wt[:, s * 2 * width : (s + 1) * 2 * width] for s in range(ns)]
    parts = [[], []]
    for s in range(0, ns, 2):
        a, b = wts[s], wts[s + 1]
        parts[0].append(jnp.where(first, a, pltpu.roll(b, width, 1)))
        parts[1].append(jnp.where(first, pltpu.roll(a, width, 1), b))
    wr, wi = (jnp.concatenate(p, axis=1) for p in parts)
    column = lax.broadcasted_iota(jnp.int32, (width, chans), 1)
    span = gates * row * GROUP // 2
    name = 2 * (column // (2 * span) * span + column % span) + column // span % 2
    eye = lax.broadcasted_iota(jnp.int32, (width, width), 0) == lax.broadcasted_iota(jnp.int32, (width, width), 1)
    rows = []
    for s in range(ns):
        line = jnp.broadcast_to(sv[s : s + 1, :].astype(F32), (width, width))
        chosen = jnp.sum(jnp.where(eye, line, 0.0), axis=1, keepdims=True)
        rows.append(jnp.where(chosen == name.astype(F32), 1.0, 0.0))
    pick = jnp.concatenate(rows, axis=0).astype(BF16)
    wr_h, wr_l = halves(wr)
    wi_h, wi_l = halves(wi)
    moved = dot(jnp.concatenate([wr_h, wr_l, wi_h, wi_l], axis=0), pick).astype(BF16)
    mr_h, mr_l, mi_h, mi_l = (moved[i * beams : (i + 1) * beams] for i in range(4))
    for q in range(nz // GROUP):
        cut = slice(q * 2 * span, (q + 1) * 2 * span)
        for half, (r, i) in enumerate(((mr_h[:, cut], mi_h[:, cut]), (mr_l[:, cut], mi_l[:, cut]))):
            steer[half, q] = jnp.concatenate(
                [jnp.concatenate([r, i], axis=1), jnp.concatenate([-i, r], axis=1)], axis=0
            )

    block = zb.at[:, pl.ds(0, gates * row), :]
    short = zb.at[:, pl.ds(0, gates * (row - 1)), :]

    def receive(z2, _):
        @pl.when(z2 == z)
        def _():
            pltpu.make_async_copy(short, short, row_sem.at[z2]).wait()

        @pl.when(z2 != z)
        def _():
            pltpu.make_async_copy(block, block, row_sem.at[z2]).wait()

        return 0

    peers = nz * row
    beam = None
    for q in (*range(1, nz // GROUP), 0):
        lax.fori_loop(q * GROUP, (q + 1) * GROUP, receive, 0)
        planes = [
            jnp.concatenate(
                [zb[plane, pl.ds(gates * q * span + g, span, stride=gates), :] for g in range(gates)], axis=1
            )
            for plane in range(4)
        ]
        data[0, q], data[1, q] = halves(jnp.concatenate(planes, axis=0))
        term = dot3((steer[0, q], steer[1, q]), (data[0, q], data[1, q]))
        beam = term if beam is None else beam + term
    out_r, out_i = beam[:beams], beam[beams:]
    power = jnp.sum(out_r * out_r + out_i * out_i, axis=1, keepdims=True)
    eye_b = lax.broadcasted_iota(jnp.int32, (beams, beams), 0) == lax.broadcasted_iota(jnp.int32, (beams, beams), 1)
    ev[0] = jnp.sum(jnp.where(eye_b, power, 0.0), axis=0, keepdims=True)
    ea[rank] = ev[0]

    def share_row(i, _):
        pltpu.make_async_remote_copy(
            src_ref=ev.at[0], dst_ref=ea.at[rank], send_sem=e_send.at[0], recv_sem=ea_sem,
            device_id=at(z, (rank + i) % row),
        ).start()
        return 0

    lax.fori_loop(1, row, share_row, 0, unroll=row - 1)

    got = [
        dot(
            pick,
            jnp.concatenate(
                [data[half, q, pl.ds(part * 2 * span, 2 * span), :] for q in range(nz // GROUP)], axis=0
            ),
        ).astype(BF16)
        for half in range(2)
        for part in range(2)
    ]
    gate_of = lax.broadcasted_iota(jnp.int32, (2 * width, got[0].shape[1]), 1) // (got[0].shape[1] // gates)
    on = jnp.where(gate_of == 0, mask[0].astype(F32), mask[1].astype(F32)).astype(BF16)
    factor = 1.0 / got[0].shape[1]
    lane_s = lax.broadcasted_iota(jnp.int32, (width, 2 * width), 1) < width
    total = jnp.zeros((beams, 2 * width), F32)

    def subarray(s):
        cut = slice(s * width, (s + 1) * width)
        high = jnp.concatenate([got[0][cut], got[1][cut]], axis=0)
        low = jnp.concatenate([got[2][cut], got[3][cut]], axis=0)
        full = dot3((high * on, low * on), (high, low), across=True) * factor
        top, turned = full[:width], pltpu.roll(full[width:], width, 1)
        cov = turned + jnp.where(lane_s, top, -top)
        cov_ref[s] = cov
        matrix = jnp.concatenate([jnp.where(lane_s, cov, -cov), pltpu.roll(cov, width, 1)], axis=0)
        return dot3(halves(wts[s]), halves(matrix)) * wts[s]

    for s in range(ns):
        total = total + subarray(s)

    ra = ea.at[pl.ds(0, row - 1)]
    pltpu.make_async_copy(ra, ra, ea_sem).wait()
    ev[1] = jnp.sum(ea[...], axis=0)
    eb[z] = ev[1]

    def share_column(i, _):
        pltpu.make_async_remote_copy(
            src_ref=ev.at[1], dst_ref=eb.at[z], send_sem=e_send.at[1], recv_sem=eb_sem,
            device_id=at((z + i) % nz, rank),
        ).start()
        return 0

    lax.fori_loop(1, nz, share_column, 0, unroll=nz - 1)

    inverse = 1.0 / jnp.sqrt(jnp.sum(total, axis=1, keepdims=True) + loading)
    pulses = out_r.shape[1] // gates
    for part, out in enumerate((out_r, out_i)):
        scaled = out * inverse
        for g in range(gates):
            filt_ref[part, pl.ds(g, beams, stride=gates), :] = scaled[:, g * pulses : (g + 1) * pulses]

    every = zb.at[:, pl.ds(0, gates * (peers - 1)), :]
    pltpu.make_async_copy(every, every, send_sem).wait()
    pltpu.make_async_copy(ra, ra, e_send.at[0]).wait()
    rb = eb.at[pl.ds(0, nz - 1)]
    pltpu.make_async_copy(rb, rb, e_send.at[1]).wait()
    pltpu.make_async_copy(rb, rb, eb_sem).wait()
    energy_ref[...] = jnp.sum(eb[...], axis=0) * (1.0 / (peers * gates * pulses))


def writer(*refs):
    sem = refs[-1]
    copies = [pltpu.make_async_copy(refs[i], refs[i + 3], sem.at[i]) for i in range(3)]
    for copy in copies:
        copy.start()
    for copy in copies:
        copy.wait()


def body(samples, beam_weights, subarrays, training):
    range_count, nc = lax.axis_size("range"), lax.axis_size("sub")
    nz = range_count // NX
    parts_iq, chan_dev, all_gates, pulses = samples.shape
    gates = training.shape[0]
    _, ns, _, width, half_beams = beam_weights.shape
    beams = half_beams * nc
    anywhere = pl.BlockSpec(memory_space=pl.ANY)
    vmem = pl.BlockSpec(memory_space=pltpu.VMEM)
    dma, regular = pltpu.SemaphoreType.DMA, pltpu.SemaphoreType.REGULAR
    cov, filt, energy = pl.pallas_call(
        functools.partial(kernel, nz, nc, gates),
        out_shape=(
            pltpu.VMEM((ns, width, 2 * width), F32),
            pltpu.VMEM((parts_iq, beams * gates, pulses), F32),
            pltpu.VMEM((1, beams), F32),
        ),
        in_specs=[anywhere] * 4,
        out_specs=(vmem, vmem, vmem),
        scratch_shapes=[
            pltpu.VMEM((parts_iq * chan_dev, all_gates, pulses), F32),
            pltpu.VMEM((parts_iq * chan_dev, all_gates, pulses), F32),
            pltpu.VMEM((nc, ns, 2, width, half_beams), F32),
            pltpu.VMEM((2, nz // GROUP, 2 * beams, 4 * NX * nc * GROUP), BF16),
            pltpu.VMEM((2, nz // GROUP, 4 * NX * nc * GROUP, gates * pulses), BF16),
            pltpu.VMEM((ns, width), jnp.int32),
            pltpu.VMEM((2, 1, beams), F32),
            pltpu.VMEM((NX * nc, 1, beams), F32),
            pltpu.VMEM((nz, 1, beams), F32),
            pltpu.SMEM((gates,), jnp.int32),
            dma((4,)),
            dma,
            dma((nz,)),
            regular((nz,)),
            dma,
            dma,
            dma((2,)),
            dma,
            dma,
        ],
        compiler_params=pltpu.CompilerParams(collective_id=1, has_side_effects=True),
    )(
        samples.reshape(parts_iq * chan_dev, all_gates, pulses),
        beam_weights,
        subarrays.reshape(ns, width),
        training,
    )
    results = tuple(pltpu.with_memory_space_constraint(r, pltpu.VMEM) for r in (cov, filt, energy))
    cov, filt, energy = pl.pallas_call(
        writer,
        out_shape=tuple(jax.ShapeDtypeStruct(r.shape, F32) for r in results),
        in_specs=[vmem] * 3,
        out_specs=(anywhere,) * 3,
        scratch_shapes=[dma((3,))],
    )(*results)
    return (
        cov.reshape(1, ns, width, 2 * width),
        filt.reshape(parts_iq, beams, gates, pulses),
        energy.reshape(beams),
    )


def solution(mesh):
    return jax.shard_map(
        body,
        mesh=mesh,
        in_specs=(
            P(None, GROUPS_RANGE_SUB, None, None),
            P(GROUPS_RANGE, None, None, None, "sub"),
            P(GROUPS_RANGE_SUB, None, None),
            P(GROUPS_RANGE_SUB),
        ),
        out_specs=(
            P(GROUPS_RANGE_SUB, None, None, None),
            P(None, None, GROUPS_RANGE_SUB, None),
            P("groups"),
        ),
        check_vma=False,
    )
```
